32 devices in a mesh: freq: 8 (over z, core), cell: 4 (over y, x).
Axes of the slice: x: 2, y: 2, z: 4, core: 2. Of those that a mesh axis runs over, the one named last changes fastest.
Arguments:
- covariance: bfloat16 [256, 2, 256, 256], P('freq', None, 'cell'), may hold values from -4 to 6, as said below
- replica: bfloat16 [256, 2, 256, 2048], P('freq', None, None, 'cell'), may hold values from -0.25 to 0.25
- transmission: bfloat16 [256, 2048], P('freq', 'cell'), may hold values from 0.29882812 to 3
Outputs:
- ambiguity: float32 [2048], P('cell')
- relative: float32 [2048], P('cell')
The draws below stay inside these ranges and needn't reach their ends.
Inputs may be any that keep to these rules, and one draw needn't show every extreme that they name: Each covariance[f, 0] + i covariance[f, 1] is exactly Hermitian, also after rounding to bfloat16; before rounding all its eigenvalues are at least 0.5.
All inputs are finite; a program needn't handle non-finite values.
Results may differ from the reference program's by a relative error of at most 0.0003.
Values may be sent and summed in bfloat16 or wider, within the bound.
A program may use at most 384 MiB of HBM per device.

```python
import math
import jax
import jax.numpy as jnp
from jax import lax

NR = 256
FREQS = 256
CELLS = 2048


def drawn(key):
    count = 3
    key_cells, key_source = jax.random.split(jax.random.fold_in(key, 41))
    span = CELLS // count
    cells = jax.random.randint(key_cells, (count,), 0, span, dtype=jnp.int32) + span * jnp.arange(count, dtype=jnp.int32)
    bound = 0.25 * (2.0 * NR) ** 0.5
    source = jax.random.truncated_normal(key_source, -bound, bound, (FREQS, 2, NR, count), jnp.float32) / (2.0 * NR) ** 0.5
    return (cells, source)


def draw_replica(key, part):
    cells, source = drawn(key)
    bound = 0.25 * (2.0 * NR) ** 0.5
    field = jax.random.truncated_normal(jax.random.fold_in(key, 43), -bound, bound, (FREQS, 2, NR, CELLS), jnp.float32) / (2.0 * NR) ** 0.5
    position = jnp.arange(CELLS, dtype=jnp.int32)
    for index in range(source.shape[3]):
        field = jnp.where(position == cells[index], source[:, :, :, index:index + 1], field)
    return field.astype(jnp.bfloat16)


def draw_covariance(key, part):
    cells, source = drawn(key)
    key_re, key_im = jax.random.split(jax.random.fold_in(key, 17), 2)
    key_power = jax.random.fold_in(key, 29)
    real = jax.random.normal(key_re, (FREQS, NR, NR), jnp.float32)
    imag = jax.random.normal(key_im, (FREQS, NR, NR), jnp.float32)
    count = source.shape[3]
    powers = jnp.exp(jax.random.uniform(key_power, (FREQS, count), jnp.float32, jnp.log(6.0), jnp.log(30.0)))
    scale = 1.0 / (2.0 * NR)
    gram_re = (jnp.einsum('fik,fjk->fij', real, real, precision=lax.Precision.HIGHEST) + jnp.einsum('fik,fjk->fij', imag, imag, precision=lax.Precision.HIGHEST)) * scale
    gram_im = (jnp.einsum('fik,fjk->fij', imag, real, precision=lax.Precision.HIGHEST) - jnp.einsum('fik,fjk->fij', real, imag, precision=lax.Precision.HIGHEST)) * scale
    part_re = source[:, 0]
    part_im = source[:, 1]
    weighted_re = part_re * powers[:, None, :]
    weighted_im = part_im * powers[:, None, :]
    signal_re = jnp.einsum('fik,fjk->fij', weighted_re, part_re, precision=lax.Precision.HIGHEST) + jnp.einsum('fik,fjk->fij', weighted_im, part_im, precision=lax.Precision.HIGHEST)
    signal_im = jnp.einsum('fik,fjk->fij', weighted_im, part_re, precision=lax.Precision.HIGHEST) - jnp.einsum('fik,fjk->fij', weighted_re, part_im, precision=lax.Precision.HIGHEST)
    mixed_re = gram_re + signal_re
    mixed_im = gram_im + signal_im
    cov_re = 0.5 * (mixed_re + jnp.swapaxes(mixed_re, 1, 2)) + 0.5 * jnp.eye(NR, dtype=jnp.float32)
    cov_im = 0.5 * (mixed_im - jnp.swapaxes(mixed_im, 1, 2))
    cov_re = jnp.clip(cov_re, -4.0, 6.0)
    cov_im = jnp.clip(cov_im, -4.0, 4.0)
    return jnp.stack([cov_re, cov_im], axis=1).astype(jnp.bfloat16)


def block_scale(own_key, dims, shards, smallest, high):
    factor_of, own = 1.0, jax.random.fold_in(own_key, 6)
    for axis_at, shards_of in shards:
        steps = jnp.exp(jax.random.uniform(jax.random.fold_in(own, axis_at), (shards_of,), jnp.float32, smallest / len(shards), high / len(shards)))
        factor_of = factor_of * jnp.repeat(steps, dims[axis_at] // shards_of).reshape([-1 if axis == axis_at else 1 for axis in range(len(dims))])
    return factor_of


def setup_inputs(seed: int = 0) -> dict:
    key_of = jax.random.split(jax.random.key(seed), 4)
    return {
        "covariance": draw_covariance(jax.random.fold_in(key_of[3], 71), 0),
        "replica": draw_replica(jax.random.fold_in(key_of[3], 71), 0),
        "transmission": jnp.clip(jnp.exp(math.log(3.0) - 2.306499 * jax.random.uniform(key_of[2], (FREQS, CELLS), jnp.float32) ** block_scale(key_of[2], (FREQS, CELLS), ((0, 8), (1, 4)), -0.2, 0.2)), 0.29882812, 3.0).astype(jnp.bfloat16),
    }


def one_frequency(items):
    cov_f, rep_f, trans_f = items
    stacked = cov_f.reshape(2 * NR, NR)
    first = jnp.dot(stacked, rep_f[0], preferred_element_type=jnp.float32)
    second = jnp.dot(stacked, rep_f[1], preferred_element_type=jnp.float32)
    image_re = first[:NR] - second[NR:]
    image_im = first[NR:] + second[:NR]
    power = jnp.sum(rep_f[0].astype(jnp.float32) * image_re + rep_f[1].astype(jnp.float32) * image_im, axis=0)
    amplitude = trans_f.astype(jnp.float32)
    return amplitude * amplitude * power


def reference(covariance, replica, transmission):
    powers = lax.map(one_frequency, (covariance, replica, transmission))
    ambiguity = jnp.sum(powers, axis=0) / jnp.float32(FREQS)
    peak = jnp.max(ambiguity)
    relative = ambiguity / jnp.maximum(peak, jnp.float32(1.0))
    return ambiguity, relative
```

```python
import functools

import jax
import jax.numpy as jnp
from jax import lax
from jax.experimental import pallas as pl
from jax.experimental.pallas import tpu as pltpu
from jax.sharding import PartitionSpec as P

MESH = pl.DeviceIdType.MESH


def quadratic(cov_piece, col_fields, row_fields):
    count, _, rows, depths = cov_piece.shape
    stacked = cov_piece.reshape(count, 2 * rows, depths)
    first = jnp.einsum(
        "fij,fjc->fic", stacked, col_fields[:, 0], preferred_element_type=jnp.float32
    )
    second = jnp.einsum(
        "fij,fjc->fic", stacked, col_fields[:, 1], preferred_element_type=jnp.float32
    )
    image_re = first[:, :rows] - second[:, rows:]
    image_im = first[:, rows:] + second[:, :rows]
    return jnp.sum(row_fields[:, 0] * image_re + row_fields[:, 1] * image_im, axis=1)


def plain(covariance, replica, transmission):
    freq_total = covariance.shape[0] * lax.axis_size("freq")
    power = quadratic(lax.all_gather(covariance, "cell", axis=2, tiled=True), replica, replica)
    amplitude = transmission.astype(jnp.float32)
    partial_value = jnp.sum(amplitude * amplitude * power, axis=0)
    partial_value = partial_value / jnp.float32(freq_total)
    ambiguity = lax.psum(partial_value, "freq")
    peak = lax.pmax(jnp.max(ambiguity), "cell")
    relative = ambiguity / jnp.maximum(peak, jnp.float32(1.0))
    return (ambiguity, relative)


def turned(z):
    half = z.shape[1] // 2
    return jnp.concatenate([z[:, half:], z[:, :half]], axis=1)


def kernel(
    freqs, group, cov_hbm, rep_hbm, trans_ref, amb_ref, rel_ref,
    cov, v, sx, sy, rx, ry, rd, s0, s1, masks, amp, acc, gath, peaks,
    cov_sem, rep_sem, send_sem, recv_sem, gsend, grecv, msend, mrecv,
):
    count, _, rows, depths = cov_hbm.shape
    groups = count // group
    pairs = group // 2
    cells = rep_hbm.shape[2]
    wide = 2 * rows
    fme = lax.axis_index("freq")
    me = lax.axis_index("cell")
    y = me // 2
    x = me % 2
    at_x = 2 * y + (1 - x)
    at_y = 2 * (1 - y) + x
    at_d = 2 * (1 - y) + (1 - x)
    partners = (at_x, at_y, at_d)

    def cov_copy(g):
        span = pl.ds(g * group, group)
        return pltpu.make_async_copy(cov_hbm.at[span], cov.at[span], cov_sem.at[g])

    def rep_copy(g):
        span = pl.ds(g * group, group)
        return pltpu.make_async_copy(rep_hbm.at[span], v.at[span], rep_sem.at[g])

    for g in range(groups):
        cov_copy(g).start()
    for g in range(groups):
        rep_copy(g).start()

    barrier = pltpu.get_barrier_semaphore()
    for partner in partners:
        pl.semaphore_signal(barrier, inc=1, device_id={"cell": partner}, device_id_type=MESH)
    for k in range(1, freqs):
        other = (fme + k) % freqs
        pl.semaphore_signal(barrier, inc=1, device_id={"freq": other}, device_id_type=MESH)

    def remote(g, which):
        span = pl.ds(g * pairs, pairs)
        if which == 0:
            source, target = sx.at[span], rx.at[span]
        elif which == 1:
            source, target = sy.at[span], ry.at[span]
        else:
            source, target = sx.at[span, 3], rd.at[span]
        return pltpu.make_async_remote_copy(
            src_ref=source,
            dst_ref=target,
            send_sem=send_sem.at[which, g],
            recv_sem=recv_sem.at[which, g],
            device_id={"cell": partners[which]},
            device_id_type=MESH,
        )

    row = lax.broadcasted_iota(jnp.int32, (rows, wide), 0)
    lane = lax.broadcasted_iota(jnp.int32, (rows, wide), 1)

    def triangle(col):
        inside = jnp.logical_and(col >= 0, col < rows)
        upper = jnp.where(col > row, 1.0, jnp.where(col == row, 0.5, 0.0))
        lower = jnp.where(col < row, 1.0, 0.0)
        zero = jnp.zeros((rows, wide), jnp.float32)
        full = jnp.where(inside, 1.0, zero)
        return full, jnp.where(inside, upper, zero), jnp.where(inside, lower, zero)

    own_set = triangle(lane - rows * x)
    oth_set = triangle(lane - rows * (1 - x))
    made = (
        own_set[0], oth_set[0], own_set[0] - own_set[2], own_set[2], oth_set[1], oth_set[2],
        own_set[1] + oth_set[0], own_set[2] + oth_set[0],
    )
    for k, mask in enumerate(made):
        masks[k] = mask.astype(jnp.bfloat16)
    amplitude = trans_ref[...].astype(jnp.float32)
    amp[...] = amplitude * amplitude
    s0[...] = jnp.zeros_like(s0)
    s1[...] = jnp.zeros_like(s1)
    acc[...] = jnp.zeros_like(acc)

    own_tile = pl.ds(pl.multiple_of(y * wide, wide), wide)
    opp_tile = pl.ds(pl.multiple_of((1 - y) * wide, wide), wide)

    def pack(p):
        own, oth = masks[0], masks[1]
        up, low = masks[2], masks[3]
        f0, f1 = 2 * p, 2 * p + 1
        a0, b0 = cov[f0, 0, :, own_tile], cov[f0, 1, :, own_tile]
        a1, b1 = cov[f1, 0, :, own_tile], cov[f1, 1, :, own_tile]
        c0, d0 = cov[f0, 0, :, opp_tile], cov[f0, 1, :, opp_tile]
        c1, d1 = cov[f1, 0, :, opp_tile], cov[f1, 1, :, opp_tile]
        p0 = a0 * up + b0 * low
        p1 = a1 * up + b1 * low
        sy[p, 0] = p0 + a0 * oth
        sy[p, 1] = p1 + a1 * oth
        sy[p, 2] = turned(b0 * oth) + b1 * oth
        sy[p, 3] = turned(c1 * oth) + d1 * oth
        sx[p, 0] = c0
        sx[p, 1] = d0
        sx[p, 2] = c1 * own + turned(d1 * own)
        sx[p, 3] = p0 + turned(p1)

    def pack_group(g):
        cov_copy(g).wait()
        for k in range(pairs):
            pack(g * pairs + k)

    def send_group(g):
        for which in range(3):
            remote(g, which).start()

    pack_group(0)
    pl.semaphore_wait(barrier, len(partners) + freqs - 1)

    def ahead(g, carry):
        pack_group(g)
        send_group(g - 1)
        return carry

    lax.fori_loop(1, groups, ahead, 0)
    send_group(groups - 1)

    def put(s, block, own_side, ta, tb):
        base = pl.multiple_of(block * rows, rows)
        tile = y if own_side else 1 - y
        first = pl.ds(base, rows)
        second = pl.ds(pl.multiple_of(depths + base, rows), rows)
        left = pl.ds(pl.multiple_of(tile * wide, wide), wide)
        right = pl.ds(pl.multiple_of(depths + tile * wide, wide), wide)
        s[first, left] = ta
        s[first, right] = -tb
        s[second, left] = tb
        s[second, right] = ta

    def build(p):
        own, oth = masks[0], masks[1]
        own_low = masks[3]
        oth_up, oth_low = masks[4], masks[5]
        own_up_oth, own_low_oth = masks[6], masks[7]
        f0, f1 = 2 * p, 2 * p + 1
        for f, s in ((f0, s0), (f1, s1)):
            put(s, me, True, cov[f, 0, :, own_tile] * own_up_oth, cov[f, 1, :, own_tile] * own_low_oth)
            put(s, me, False, cov[f, 0, :, opp_tile], cov[f, 1, :, opp_tile])
        diag = rx[p, 3]
        put(s0, at_x, True, diag * oth_up, diag * oth_low)
        put(s0, at_x, False, rx[p, 0], rx[p, 1])
        diag = turned(diag)
        put(s1, at_x, True, diag * oth_up, diag * oth_low)
        block = rx[p, 2]
        put(s1, at_x, False, block * oth, turned(block * own))
        b_both = ry[p, 2]
        block = ry[p, 0]
        put(s0, at_y, False, block * own_up_oth, block * own_low + turned(b_both * own))
        block = ry[p, 1]
        put(s1, at_y, False, block * own_up_oth, block * own_low + b_both * oth)
        block = ry[p, 3]
        put(s1, at_y, True, turned(block * own), block * oth)
        diag = rd[p]
        put(s0, at_d, False, diag * oth_up, diag * oth_low)
        diag = turned(diag)
        put(s1, at_d, False, diag * oth_up, diag * oth_low)

    part = 256 if cells % 256 == 0 else cells

    def apply(f, s):
        for c in range(0, cells, part):
            field = v[f, :, c:c + part]
            image = jnp.dot(s[...], field, preferred_element_type=jnp.float32)
            product = image * field.astype(jnp.float32)
            folded = jnp.sum(product.reshape(2 * depths // 8, 8, part), axis=0)
            acc[:, c:c + part] += folded * amp[pl.ds(f, 1), c:c + part]

    def step(g, carry):
        rep_copy(g).wait()
        for which in range(3):
            remote(g, which).wait_recv()

        def pair(k, inner):
            p = g * pairs + k
            build(p)
            apply(2 * p, s0)
            apply(2 * p + 1, s1)
            return inner

        return lax.fori_loop(0, pairs, pair, carry)

    lax.fori_loop(0, groups, step, 0)

    scale = 2.0 / (count * freqs)
    gath[fme] = jnp.sum(acc[...], axis=0, keepdims=True) * scale

    def drain(g, carry):
        for which in range(3):
            remote(g, which).wait_send()
        return carry

    lax.fori_loop(0, groups, drain, 0)

    def share(k):
        other = (fme + k) % freqs
        return pltpu.make_async_remote_copy(
            src_ref=gath.at[fme], dst_ref=gath.at[fme],
            send_sem=gsend.at[k], recv_sem=grecv.at[k],
            device_id={"freq": other}, device_id_type=MESH,
        )

    for k in range(1, freqs):
        share(k).start()
    for k in range(1, freqs):
        share(k).wait_recv()
    total = gath[0]
    for k in range(1, freqs):
        total = total + gath[k]
    amb_ref[...] = total
    top = jnp.max(total, axis=1, keepdims=True)
    peaks[3] = jnp.broadcast_to(top, (1, 128))
    sent = []
    for k, partner in enumerate(partners):
        copy = pltpu.make_async_remote_copy(
            src_ref=peaks.at[3], dst_ref=peaks.at[k],
            send_sem=msend.at[k], recv_sem=mrecv.at[k],
            device_id={"cell": partner}, device_id_type=MESH,
        )
        copy.start()
        sent.append(copy)
    for k in range(1, freqs):
        share(k).wait_send()
    for copy in sent:
        copy.wait()
    best = jnp.max(jnp.max(peaks[...], axis=0), axis=1, keepdims=True)
    rel_ref[...] = total / jnp.maximum(best, 1.0)


def fused(freqs, group, covariance, replica, transmission):
    count, _, rows, depths = covariance.shape
    cells = replica.shape[3]
    fields = replica.reshape(count, 2 * depths, cells)
    groups = count // group
    wide = 2 * rows
    bf, f32 = jnp.bfloat16, jnp.float32
    dma = pltpu.SemaphoreType.DMA
    vm = pltpu.VMEM
    amb, rel = pl.pallas_call(
        functools.partial(kernel, freqs, group),
        out_shape=[jax.ShapeDtypeStruct((1, cells), f32)] * 2,
        in_specs=[
            pl.BlockSpec(memory_space=pl.ANY),
            pl.BlockSpec(memory_space=pl.ANY),
            pl.BlockSpec(memory_space=pltpu.VMEM),
        ],
        out_specs=[pl.BlockSpec(memory_space=pltpu.VMEM)] * 2,
        scratch_shapes=[
            vm((count, 2, rows, depths), bf),
            vm((count, 2 * depths, cells), bf),
            vm((count // 2, 4, rows, wide), bf),
            vm((count // 2, 4, rows, wide), bf),
            vm((count // 2, 4, rows, wide), bf),
            vm((count // 2, 4, rows, wide), bf),
            vm((count // 2, rows, wide), bf),
            vm((2 * depths, 2 * depths), bf),
            vm((2 * depths, 2 * depths), bf),
            vm((8, rows, wide), bf),
            vm((count, cells), f32),
            vm((8, cells), f32),
            vm((freqs, 1, cells), f32),
            vm((4, 1, 128), f32),
            dma((groups,)),
            dma((groups,)),
            dma((3, groups)),
            dma((3, groups)),
            dma((freqs,)),
            dma((freqs,)),
            dma((3,)),
            dma((3,)),
        ],
        compiler_params=pltpu.CompilerParams(
            collective_id=0, has_side_effects=True, vmem_limit_bytes=60 * 1024 * 1024
        ),
    )(covariance, fields, transmission)
    return amb.reshape(cells), rel.reshape(cells)


def solution(mesh):
    freqs = mesh.shape["freq"]
    four = mesh.shape["cell"] == 4

    def shards(covariance, replica, transmission):
        count, _, rows, _ = covariance.shape
        if four and freqs > 1 and rows == 64 and count % 4 == 0 and replica.shape[3] % 128 == 0:
            return fused(freqs, 4, covariance, replica, transmission)
        return plain(covariance, replica, transmission)

    return jax.shard_map(
        shards,
        mesh=mesh,
        in_specs=(P("freq", None, "cell", None), P("freq", None, None, "cell"), P("freq", "cell")),
        out_specs=(P("cell"), P("cell")),
        check_vma=False,
    )
```

```python
import functools

import jax
import jax.numpy as jnp
from jax import lax
from jax.experimental import pallas as pl
from jax.experimental.pallas import tpu as pltpu
from jax.sharding import PartitionSpec as P

MESH = pl.DeviceIdType.MESH


def quadratic(cov_piece, col_fields, row_fields):
    count, _, rows, depths = cov_piece.shape
    stacked = cov_piece.reshape(count, 2 * rows, depths)
    first = jnp.einsum(
        "fij,fjc->fic", stacked, col_fields[:, 0], preferred_element_type=jnp.float32
    )
    second = jnp.einsum(
        "fij,fjc->fic", stacked, col_fields[:, 1], preferred_element_type=jnp.float32
    )
    image_re = first[:, :rows] - second[:, rows:]
    image_im = first[:, rows:] + second[:, :rows]
    return jnp.sum(row_fields[:, 0] * image_re + row_fields[:, 1] * image_im, axis=1)


def plain(covariance, replica, transmission):
    freq_total = covariance.shape[0] * lax.axis_size("freq")
    power = quadratic(lax.all_gather(covariance, "cell", axis=2, tiled=True), replica, replica)
    amplitude = transmission.astype(jnp.float32)
    partial_value = jnp.sum(amplitude * amplitude * power, axis=0)
    partial_value = partial_value / jnp.float32(freq_total)
    ambiguity = lax.psum(partial_value, "freq")
    peak = lax.pmax(jnp.max(ambiguity), "cell")
    relative = ambiguity / jnp.maximum(peak, jnp.float32(1.0))
    return (ambiguity, relative)


def turned(z):
    half = z.shape[1] // 2
    return jnp.concatenate([z[:, half:], z[:, :half]], axis=1)


def kernel(
    freqs, group, cov_hbm, rep_hbm, trans_ref, amb_ref, rel_ref,
    cov, v, sx, sy, rx, ry, rd, s0, s1, masks, amp, acc, gath, peaks,
    cov_sem, rep_sem, send_sem, recv_sem, gsend, grecv, msend, mrecv,
):
    count, _, rows, depths = cov_hbm.shape
    groups = count // group
    pairs = group // 2
    cells = rep_hbm.shape[2]
    wide = 2 * rows
    fme = lax.axis_index("freq")
    me = lax.axis_index("cell")
    y = me // 2
    x = me % 2
    at_x = 2 * y + (1 - x)
    at_y = 2 * (1 - y) + x
    at_d = 2 * (1 - y) + (1 - x)
    partners = (at_x, at_y, at_d)

    def cov_copy(g):
        span = pl.ds(g * group, group)
        return pltpu.make_async_copy(cov_hbm.at[span], cov.at[span], cov_sem.at[g])

    def rep_copy(g):
        span = pl.ds(g * group, group)
        return pltpu.make_async_copy(rep_hbm.at[span], v.at[span], rep_sem.at[g])

    for g in range(groups):
        cov_copy(g).start()
    for g in range(groups):
        rep_copy(g).start()

    barrier = pltpu.get_barrier_semaphore()
    for partner in partners:
        pl.semaphore_signal(barrier, inc=1, device_id={"cell": partner}, device_id_type=MESH)
    for k in range(1, freqs):
        other = (fme + k) % freqs
        pl.semaphore_signal(barrier, inc=1, device_id={"freq": other}, device_id_type=MESH)

    def remote(g, which):
        span = pl.ds(g * pairs, pairs)
        if which == 0:
            source, target = sx.at[span], rx.at[span]
        elif which == 1:
            source, target = sy.at[span], ry.at[span]
        elif which == 2:
            source, target = rx.at[g * pairs, 3], rd.at[g * pairs]
        else:
            source, target = ry.at[g * pairs + 1, 0], rd.at[g * pairs + 1]
        return pltpu.make_async_remote_copy(
            src_ref=source,
            dst_ref=target,
            send_sem=send_sem.at[which, g],
            recv_sem=recv_sem.at[which, g],
            device_id={"cell": at_x if which in (0, 3) else at_y},
            device_id_type=MESH,
        )

    row = lax.broadcasted_iota(jnp.int32, (rows, wide), 0)
    lane = lax.broadcasted_iota(jnp.int32, (rows, wide), 1)

    def triangle(col):
        inside = jnp.logical_and(col >= 0, col < rows)
        upper = jnp.where(col > row, 1.0, jnp.where(col == row, 0.5, 0.0))
        lower = jnp.where(col < row, 1.0, 0.0)
        zero = jnp.zeros((rows, wide), jnp.float32)
        full = jnp.where(inside, 1.0, zero)
        return full, jnp.where(inside, upper, zero), jnp.where(inside, lower, zero)

    own_set = triangle(lane - rows * x)
    oth_set = triangle(lane - rows * (1 - x))
    made = (
        own_set[0], oth_set[0], own_set[0] - own_set[2], own_set[2], oth_set[1], oth_set[2],
        own_set[1] + oth_set[0], own_set[2] + oth_set[0], own_set[1],
    )
    for k, mask in enumerate(made):
        masks[k] = mask.astype(jnp.bfloat16)
    amplitude = trans_ref[...].astype(jnp.float32)
    amp[...] = amplitude * amplitude
    s0[...] = jnp.zeros_like(s0)
    s1[...] = jnp.zeros_like(s1)
    acc[...] = jnp.zeros_like(acc)

    own_tile = pl.ds(pl.multiple_of(y * wide, wide), wide)
    opp_tile = pl.ds(pl.multiple_of((1 - y) * wide, wide), wide)

    def pack(p):
        own, oth = masks[0], masks[1]
        up, low = masks[2], masks[3]
        f0, f1 = 2 * p, 2 * p + 1
        a0, b0 = cov[f0, 0, :, own_tile], cov[f0, 1, :, own_tile]
        a1, b1 = cov[f1, 0, :, own_tile], cov[f1, 1, :, own_tile]
        c0, d0 = cov[f0, 0, :, opp_tile], cov[f0, 1, :, opp_tile]
        c1, d1 = cov[f1, 0, :, opp_tile], cov[f1, 1, :, opp_tile]
        p0 = a0 * up + b0 * low
        p1 = a1 * up + b1 * low
        diag = p0 + turned(p1)
        sy[p, 0] = diag
        sy[p, 1] = turned(a0 * oth) + a1 * oth
        sy[p, 2] = turned(b0 * oth) + b1 * oth
        sy[p, 3] = turned(c1 * oth) + d1 * oth
        sx[p, 0] = c0
        sx[p, 1] = d0
        sx[p, 2] = c1 * own + turned(d1 * own)
        sx[p, 3] = diag

    def pack_group(g):
        cov_copy(g).wait()
        for k in range(pairs):
            pack(g * pairs + k)

    def send_group(g):
        for which in range(2):
            remote(g, which).start()

    pack_group(0)
    pl.semaphore_wait(barrier, len(partners) + freqs - 1)
    pack_group(1)
    send_group(0)
    pack_group(2)
    send_group(1)

    def put(s, block, own_side, ta, tb):
        base = pl.multiple_of(block * rows, rows)
        tile = y if own_side else 1 - y
        first = pl.ds(base, rows)
        second = pl.ds(pl.multiple_of(depths + base, rows), rows)
        left = pl.ds(pl.multiple_of(tile * wide, wide), wide)
        right = pl.ds(pl.multiple_of(depths + tile * wide, wide), wide)
        s[first, left] = ta
        s[first, right] = -tb
        s[second, left] = tb
        s[second, right] = ta

    def build(p):
        own, oth = masks[0], masks[1]
        own_low = masks[3]
        oth_up, oth_low = masks[4], masks[5]
        own_up_oth, own_low_oth = masks[6], masks[7]
        f0, f1 = 2 * p, 2 * p + 1
        for f, s in ((f0, s0), (f1, s1)):
            put(s, me, True, cov[f, 0, :, own_tile] * own_up_oth, cov[f, 1, :, own_tile] * own_low_oth)
            put(s, me, False, cov[f, 0, :, opp_tile], cov[f, 1, :, opp_tile])
        diag = rx[p, 3]
        put(s0, at_x, True, diag * oth_up, diag * oth_low)
        put(s0, at_x, False, rx[p, 0], rx[p, 1])
        diag = turned(diag)
        put(s1, at_x, True, diag * oth_up, diag * oth_low)
        block = rx[p, 2]
        put(s1, at_x, False, block * oth, turned(block * own))
        own_up = masks[8]
        a_both, b_both = ry[p, 1], ry[p, 2]
        diag = ry[p, 0]
        put(s0, at_y, False, diag * own_up + turned(a_both * own), diag * own_low + turned(b_both * own))
        diag = turned(diag)
        put(s1, at_y, False, diag * own_up + a_both * oth, diag * own_low + b_both * oth)
        block = ry[p, 3]
        put(s1, at_y, True, turned(block * own), block * oth)
        diag = rd[p]
        put(s0, at_d, False, diag * oth_up, diag * oth_low)
        diag = turned(diag)
        put(s1, at_d, False, diag * oth_up, diag * oth_low)

    part = 256 if cells % 256 == 0 else cells

    def apply(f, s):
        for c in range(0, cells, part):
            field = v[f, :, c:c + part]
            image = jnp.dot(s[...], field, preferred_element_type=jnp.float32)
            product = image * field.astype(jnp.float32)
            folded = jnp.sum(product.reshape(2 * depths // 8, 8, part), axis=0)
            acc[:, c:c + part] += folded * amp[pl.ds(f, 1), c:c + part]

    def work(g):
        rep_copy(g).wait()
        remote(g, 2).wait_recv()
        remote(g, 3).wait_recv()

        def pair(k, inner):
            p = g * pairs + k
            build(p)
            apply(2 * p, s0)
            apply(2 * p + 1, s1)
            return inner

        lax.fori_loop(0, pairs, pair, 0)

    def pass_on(g):
        remote(g, 0).wait_recv()
        remote(g, 2).start()
        remote(g, 1).wait_recv()
        remote(g, 3).start()

    def step(g, carry):
        pass_on(g)

        @pl.when(g + 2 < groups)
        def _():
            send_group(g + 2)

        @pl.when(g + 3 < groups)
        def _():
            pack_group(g + 3)

        @pl.when(g > 0)
        def _():
            work(g - 1)

        return carry

    lax.fori_loop(0, groups, step, 0)
    work(groups - 1)

    scale = 2.0 / (count * freqs)
    gath[fme] = jnp.sum(acc[...], axis=0, keepdims=True) * scale

    def drain(g, carry):
        for which in range(4):
            remote(g, which).wait_send()
        return carry

    lax.fori_loop(0, groups, drain, 0)

    def share(k):
        other = (fme + k) % freqs
        return pltpu.make_async_remote_copy(
            src_ref=gath.at[fme], dst_ref=gath.at[fme],
            send_sem=gsend.at[k], recv_sem=grecv.at[k],
            device_id={"freq": other}, device_id_type=MESH,
        )

    for k in range(1, freqs):
        share(k).start()
    for k in range(1, freqs):
        share(k).wait_recv()
    total = gath[0]
    for k in range(1, freqs):
        total = total + gath[k]
    amb_ref[...] = total
    top = jnp.max(total, axis=1, keepdims=True)
    peaks[3] = jnp.broadcast_to(top, (1, 128))
    sent = []
    for k, partner in enumerate(partners):
        copy = pltpu.make_async_remote_copy(
            src_ref=peaks.at[3], dst_ref=peaks.at[k],
            send_sem=msend.at[k], recv_sem=mrecv.at[k],
            device_id={"cell": partner}, device_id_type=MESH,
        )
        copy.start()
        sent.append(copy)
    for k in range(1, freqs):
        share(k).wait_send()
    for copy in sent:
        copy.wait()
    best = jnp.max(jnp.max(peaks[...], axis=0), axis=1, keepdims=True)
    rel_ref[...] = total / jnp.maximum(best, 1.0)


def fused(freqs, group, covariance, replica, transmission):
    count, _, rows, depths = covariance.shape
    cells = replica.shape[3]
    fields = replica.reshape(count, 2 * depths, cells)
    groups = count // group
    wide = 2 * rows
    bf, f32 = jnp.bfloat16, jnp.float32
    dma = pltpu.SemaphoreType.DMA
    vm = pltpu.VMEM
    amb, rel = pl.pallas_call(
        functools.partial(kernel, freqs, group),
        out_shape=[jax.ShapeDtypeStruct((1, cells), f32)] * 2,
        in_specs=[
            pl.BlockSpec(memory_space=pl.ANY),
            pl.BlockSpec(memory_space=pl.ANY),
            pl.BlockSpec(memory_space=pltpu.VMEM),
        ],
        out_specs=[pl.BlockSpec(memory_space=pltpu.VMEM)] * 2,
        scratch_shapes=[
            vm((count, 2, rows, depths), bf),
            vm((count, 2 * depths, cells), bf),
            vm((count // 2, 4, rows, wide), bf),
            vm((count // 2, 4, rows, wide), bf),
            vm((count // 2, 4, rows, wide), bf),
            vm((count // 2, 4, rows, wide), bf),
            vm((count // 2, rows, wide), bf),
            vm((2 * depths, 2 * depths), bf),
            vm((2 * depths, 2 * depths), bf),
            vm((9, rows, wide), bf),
            vm((count, cells), f32),
            vm((8, cells), f32),
            vm((freqs, 1, cells), f32),
            vm((4, 1, 128), f32),
            dma((groups,)),
            dma((groups,)),
            dma((4, groups)),
            dma((4, groups)),
            dma((freqs,)),
            dma((freqs,)),
            dma((3,)),
            dma((3,)),
        ],
        compiler_params=pltpu.CompilerParams(
            collective_id=0, has_side_effects=True, vmem_limit_bytes=60 * 1024 * 1024
        ),
    )(covariance, fields, transmission)
    return amb.reshape(cells), rel.reshape(cells)


def solution(mesh):
    freqs = mesh.shape["freq"]
    four = mesh.shape["cell"] == 4

    def shards(covariance, replica, transmission):
        count, _, rows, _ = covariance.shape
        if four and freqs > 1 and rows == 64 and count % 4 == 0 and count >= 12 and replica.shape[3] % 128 == 0:
            return fused(freqs, 4, covariance, replica, transmission)
        return plain(covariance, replica, transmission)

    return jax.shard_map(
        shards,
        mesh=mesh,
        in_specs=(P("freq", None, "cell", None), P("freq", None, None, "cell"), P("freq", "cell")),
        out_specs=(P("cell"), P("cell")),
        check_vma=False,
    )
```
